32 devices in a mesh: layer: 4 (over z), latent: 8 (over y, x, core).
Axes of the slice: x: 2, y: 2, z: 4, core: 2. Of those that a mesh axis runs over, the one named last changes fastest.
Arguments:
- acts: float32 [4, 64, 2304], P('layer', 'latent'), may hold values from -6 to 6
- w_enc: float32 [4, 2304, 2048], P('layer', None, 'latent'), may hold values from -0.0625 to 0.0625
- b_enc: float32 [2048], P('latent'), may hold values from -3 to 3
- w_dec: float32 [2048, 4, 2304], P('latent', 'layer'), may hold values from -0.125 to 0.125
- b_dec: float32 [4, 2304], P('layer'), may hold values from -3 to 3
Outputs:
- grad_enc: float32 [4, 2304, 2048], P('layer', None, 'latent')
- grad_benc: float32 [2048], P('latent')
The draws below stay inside these ranges and needn't reach their ends.
All inputs are finite; a program needn't handle non-finite values.
Results may differ from the reference program's by a relative error of at most 0.000076.
Values sent between devices are 32-bit elements; how exact they have to be, the bound alone decides.
No kernel may reach another device: no remote copies, remote signals or barrier semaphores. Data moves between devices by JAX's collectives and lax.ppermute only.
A program may use at most 64 MiB of HBM per device.

```python
import jax
import jax.numpy as jnp
from jax import lax

D = 2304
H = 2048
LAYERS = 4
TOKENS = 64


def shard_levels(rng, dims, split, least, high):
    factor_of, own = 1.0, jax.random.fold_in(rng, 6)
    for axis_at, blocks in split:
        steps = jnp.exp(jax.random.uniform(jax.random.fold_in(own, axis_at), (blocks,), jnp.float32, least / len(split), high / len(split)))
        factor_of = factor_of * jnp.repeat(steps, dims[axis_at] // blocks).reshape([-1 if axis == axis_at else 1 for axis in range(len(dims))])
    return factor_of


def bell_draw(rng, shape, width, most, cuts=(), dtype=jnp.bfloat16):
    values = jax.random.normal(rng, shape, jnp.float32) * width
    if len(cuts) > 0:
        values = shard_levels(rng, shape, cuts, -0.22, 0.18) * values
    return jnp.clip(values, min=-most, max=most).astype(dtype)


def setup_inputs(seed: int = 0) -> dict:
    key_list = jax.random.split(jax.random.key(seed), 6)
    return {
        "acts": bell_draw(key_list[0], (LAYERS, TOKENS, D), 1.0, 6.0, ((0, 4), (1, 8)), jnp.float32),
        "w_enc": bell_draw(key_list[1], (LAYERS, D, H), (LAYERS * D) ** -0.5, 0.0625, ((0, 4), (2, 8)), jnp.float32),
        "b_enc": bell_draw(key_list[2], (H,), 0.5, 3.0, ((0, 8),), jnp.float32),
        "w_dec": bell_draw(key_list[3], (H, LAYERS, D), H ** -0.5, 0.125, ((0, 8), (1, 4)), jnp.float32),
        "b_dec": bell_draw(key_list[4], (LAYERS, D), 0.5, 3.0, ((0, 4),), jnp.float32),
    }


SHARP = 4.0

def reference(acts, w_enc, b_enc, w_dec, b_dec):
    high = lax.Precision.HIGHEST
    pre = jnp.einsum('ltd,ldh->th', acts, w_enc, precision=high) + b_enc[None, :]
    codes = jax.nn.softplus(SHARP * pre) / SHARP
    recon = jnp.einsum('th,hld->ltd', codes, w_dec, precision=high) + b_dec[:, None, :]
    resid = recon - acts
    dec_norm = lax.optimization_barrier(jnp.sum(jnp.sqrt(lax.optimization_barrier(jnp.sum(w_dec * w_dec, axis=2))), axis=1))
    code_grad = jnp.einsum('ltd,hld->th', resid, w_dec, precision=high) + dec_norm[None, :]
    pre_grad = code_grad * jax.nn.sigmoid(SHARP * pre)
    grad_enc = jnp.einsum('ltd,th->ldh', acts, pre_grad, precision=high)
    grad_benc = lax.optimization_barrier(jnp.sum(pre_grad, axis=0))
    return (grad_enc, grad_benc)
```

```python
import jax
import jax.numpy as jnp
from jax import lax
from jax.sharding import PartitionSpec as P

SHARP = 4.0
DIRECT_MAX = 8


def dot(a, b, dims):
    return lax.dot_general(
        a, b, (dims, ((), ())), precision=lax.Precision.HIGH, preferred_element_type=jnp.float32
    )


def on_device(layers, latents, acts, w_enc, b_enc, w_dec, b_dec):
    chips = latents // 2
    direct = chips <= DIRECT_MAX and chips & (chips - 1) == 0
    same_core = [[2 * j + c for j in range(chips)] for c in range(2)]

    def to_partner(x):
        return lax.ppermute(x, "latent", [(i, i ^ 1) for i in range(latents)])

    def to_chip(x, k):
        return lax.ppermute(x, "latent", [(i, i ^ (2 * k)) for i in range(latents)])

    def gather_chips(x):
        if direct:
            return jnp.concatenate([x] + [to_chip(x, k) for k in range(1, chips)], axis=0)
        return lax.all_gather(x, "latent", axis=0, tiled=True, axis_index_groups=same_core)

    def scatter_chips(x, rows):
        if direct:
            total = x[:rows]
            for k in range(1, chips):
                total = total + to_chip(x[k * rows : (k + 1) * rows], k)
            return total
        return lax.psum_scatter(
            x, "latent", scatter_dimension=0, tiled=True, axis_index_groups=same_core
        )

    def sum_layers(x):
        total = x
        for k in range(1, layers):
            total = total + lax.ppermute(
                x, "layer", [(i, (i + k) % layers) for i in range(layers)]
            )
        return total

    own_enc, own_dec, offset, local = w_enc[0], w_dec[:, 0, :], b_dec[0], acts[0]
    rows, width = local.shape[0], own_enc.shape[1]
    other_enc = to_partner(own_enc)
    other_bias = to_partner(b_enc)
    bias = jnp.concatenate([b_enc, other_bias])
    gathered = gather_chips(local)
    other_dec = to_partner(own_dec)
    other_gathered = to_partner(gathered)
    norms = jnp.concatenate(
        [jnp.sqrt(jnp.sum(w * w, axis=1)) for w in (own_dec, other_dec)]
    )
    partial = jnp.concatenate(
        [dot(gathered, w, ((1,), (0,))) for w in (own_enc, other_enc)], axis=1
    )
    pre = sum_layers(partial) + bias[None, :]
    codes = jax.nn.softplus(SHARP * pre) / SHARP
    gate = jax.nn.sigmoid(SHARP * pre)
    recon = scatter_chips(
        dot(codes[:, :width], own_dec, ((1,), (0,)))
        + dot(codes[:, width:], other_dec, ((1,), (0,))),
        rows,
    )
    resid = gather_chips(recon + offset[None, :] - local)
    grad_part = jnp.concatenate(
        [dot(resid, w, ((1,), (1,))) for w in (own_dec, other_dec)], axis=1
    )
    code_grad = sum_layers(grad_part + norms[None, :])
    pre_grad = code_grad * gate
    mine = pre_grad[:, :width]
    theirs = to_partner(pre_grad[:, width:])
    tokens = jnp.concatenate([gathered, other_gathered], axis=0)
    all_grad = jnp.concatenate([mine, theirs], axis=0)
    grad = dot(tokens, all_grad, ((0,), (0,)))
    return (grad[None, :, :], jnp.sum(all_grad, axis=0))


def solution(mesh):
    layers, latents = mesh.shape["layer"], mesh.shape["latent"]

    def body(*args):
        return on_device(layers, latents, *args)

    return jax.shard_map(
        body,
        mesh=mesh,
        in_specs=(
            P("layer", "latent", None),
            P("layer", None, "latent"),
            P("latent"),
            P("latent", "layer", None),
            P("layer", None),
        ),
        out_specs=(P("layer", None, "latent"), P("latent")),
        check_vma=False,
    )
```

```python
import functools

import jax
import jax.numpy as jnp
from jax import lax
from jax.experimental import pallas as pl
from jax.experimental.pallas import tpu as pltpu
from jax.sharding import PartitionSpec as P

SHARP = 4.0
DIRECT_MAX = 8
CHUNK = 256
F32, BF16 = jnp.float32, jnp.bfloat16


def split(x):
    high = x.astype(BF16)
    return high, (x - high.astype(F32)).astype(BF16)


def stacked(x):
    return jnp.concatenate(split(x), axis=0)


def dot(a, b, dims):
    return lax.dot_general(a, b, (dims, ((), ())), preferred_element_type=F32)


def fold(x):
    half = x.shape[0] // 2
    return x[:half] + x[half:]


def call(kernel, outs, args, flops, name):
    outs = tuple(jax.ShapeDtypeStruct(*o) for o in outs)
    moved = sum(a.size * a.dtype.itemsize for a in args + outs)
    return pl.pallas_call(
        kernel,
        out_shape=outs,
        in_specs=[pl.BlockSpec(memory_space=pltpu.VMEM)] * len(args),
        out_specs=[pl.BlockSpec(memory_space=pltpu.VMEM)] * len(outs),
        compiler_params=pltpu.CompilerParams(vmem_limit_bytes=30 * 2**20),
        cost_estimate=pl.CostEstimate(flops=flops, bytes_accessed=moved, transcendentals=0),
        name=name,
    )(*args)


def rows_of(refs):
    return jnp.concatenate([r[...] for r in refs], axis=0) if len(refs) > 1 else refs[0][...]


def encode_kernel(n, *refs):
    blocks, weights, out = refs[:n], refs[n:-1], refs[-1]
    left = stacked(rows_of(blocks))
    width = weights[0].shape[1]
    for at, w in enumerate(weights):
        total = None
        for start in range(0, w.shape[0], CHUNK):
            part = left[:, start : start + CHUNK]
            for right in split(w[start : start + CHUNK, :]):
                term = dot(part, right, ((1,), (0,)))
                total = term if total is None else total + term
        out[:, at * width : (at + 1) * width] = fold(total)


def prepare_kernel(own, other, high, low, norms):
    rows = own.shape[0]
    for at, w in enumerate((own, other)):
        for start in range(0, rows, 32):
            x = w[start : start + 32, 0, :]
            here = slice(at * rows + start, at * rows + start + 32)
            high[here, :], low[here, :] = split(x)
            norms[here, :] = jnp.sqrt(jnp.sum(x * x, axis=1, keepdims=True))


def decode_kernel(n, *refs):
    parts, (bias, high, low), (out, gate) = refs[:n], refs[n:-2], refs[-2:]
    pre = parts[0][...]
    for p in parts[1:]:
        pre = pre + p[...]
    scaled = SHARP * (pre + bias[...])
    decay = jnp.exp(-jnp.abs(scaled))
    codes = (jnp.maximum(scaled, 0.0) + jnp.log1p(decay)) / SHARP
    gate[...] = jnp.where(scaled >= 0, 1.0, decay) / (1.0 + decay)
    left = stacked(codes)
    for start in range(0, high.shape[1], CHUNK):
        here = slice(start, start + CHUNK)
        out[:, here] = fold(
            dot(left, high[:, here], ((1,), (0,))) + dot(left, low[:, here], ((1,), (0,)))
        )


def gradient_kernel(n, *refs):
    blocks, (high, low, norms, out) = refs[:n], refs[n:]
    left = stacked(rows_of(blocks))
    width = high.shape[0] // 2
    for at in range(2):
        here = slice(at * width, (at + 1) * width)
        total = dot(left, high[here, :], ((1,), (1,))) + dot(left, low[here, :], ((1,), (1,)))
        out[:, here] = fold(total) + norms[:, here]


def turn_kernel(n, *refs):
    own, (other, out) = refs[:n], refs[n:]
    x = jnp.concatenate([rows_of(own), other[...]], axis=0)
    high, low = split(x)
    out[...] = jnp.concatenate([high, low, high, low], axis=0).T


def weight_kernel(turned, mine, theirs, out, bias, right):
    @pl.when(pl.program_id(0) == 0)
    def _():
        grad = jnp.concatenate([mine[...], theirs[...]], axis=0)
        bias[...] = jnp.sum(grad, axis=0, keepdims=True)
        high, low = split(grad)
        right[...] = jnp.concatenate([high, high, low, low], axis=0)

    out[...] = dot(turned[...], right[...], ((1,), (0,)))


def weight_gradient(turned, mine, theirs):
    features, depth = turned.shape
    tokens, width = mine.shape
    steps = 4
    tile = features // steps
    return pl.pallas_call(
        weight_kernel,
        grid=(steps,),
        out_shape=(
            jax.ShapeDtypeStruct((features, width), F32),
            jax.ShapeDtypeStruct((1, width), F32),
        ),
        in_specs=[
            pl.BlockSpec((tile, depth), lambda i: (i, 0)),
            pl.BlockSpec((tokens, width), lambda i: (0, 0)),
            pl.BlockSpec((tokens, width), lambda i: (0, 0)),
        ],
        out_specs=[
            pl.BlockSpec((tile, width), lambda i: (i, 0)),
            pl.BlockSpec((1, width), lambda i: (0, 0)),
        ],
        scratch_shapes=[pltpu.VMEM((depth, width), BF16)],
        compiler_params=pltpu.CompilerParams(vmem_limit_bytes=30 * 2**20),
        cost_estimate=pl.CostEstimate(
            flops=2 * features * depth * width,
            bytes_accessed=features * (depth * 2 + width * 4),
            transcendentals=0,
        ),
        name="weight_gradient",
    )(turned, mine, theirs)


def on_device(layers, latents, acts, w_enc, b_enc, w_dec, b_dec):
    chips = latents // 2
    direct = chips <= DIRECT_MAX and chips & (chips - 1) == 0
    same_core = [[2 * j + c for j in range(chips)] for c in range(2)]

    def to_partner(x):
        return lax.ppermute(x, "latent", [(i, i ^ 1) for i in range(latents)])

    def to_chip(x, k):
        return lax.ppermute(x, "latent", [(i, i ^ (2 * k)) for i in range(latents)])

    def gather_chips(x):
        if direct:
            return [x] + [to_chip(x, k) for k in range(1, chips)]
        return [lax.all_gather(x, "latent", axis=0, tiled=True, axis_index_groups=same_core)]

    def scatter_chips(x, rows):
        if direct:
            total = x[:rows]
            for k in range(1, chips):
                total = total + to_chip(x[k * rows : (k + 1) * rows], k)
            return total
        return lax.psum_scatter(
            x, "latent", scatter_dimension=0, tiled=True, axis_index_groups=same_core
        )

    def from_layers(x):
        return [x] + [
            lax.ppermute(x, "layer", [(i, (i + k) % layers) for i in range(layers)])
            for k in range(1, layers)
        ]

    own_enc, offset, local = w_enc[0], b_dec[0], acts[0]
    rows, features = local.shape
    width = own_enc.shape[1]
    tokens = rows * chips
    work = 4 * 2 * tokens * features * 2 * width

    other_enc = to_partner(own_enc)
    other_bias = to_partner(b_enc)
    bias = jnp.concatenate([b_enc, other_bias])[None, :]
    gathered = gather_chips(local)
    other_dec = to_partner(w_dec)
    (partial,) = call(
        functools.partial(encode_kernel, len(gathered)),
        [((tokens, 2 * width), F32)],
        (*gathered, own_enc, other_enc),
        work,
        "encode",
    )
    high, low, norms = call(
        prepare_kernel,
        [((2 * width, features), BF16), ((2 * width, features), BF16), ((2 * width, 1), F32)],
        (w_dec, other_dec),
        work,
        "prepare",
    )
    norms = norms.reshape(1, 2 * width)
    other_gathered = to_partner(
        jnp.concatenate(gathered, axis=0) if len(gathered) > 1 else gathered[0]
    )
    (turned,) = call(
        functools.partial(turn_kernel, len(gathered)),
        [((features, 8 * tokens), BF16)],
        (*gathered, other_gathered),
        work,
        "turn",
    )
    parts = from_layers(partial)
    recon, gate = call(
        functools.partial(decode_kernel, len(parts)),
        [((tokens, features), F32), ((tokens, 2 * width), F32)],
        (*parts, bias, high, low),
        work,
        "decode",
    )
    resid = scatter_chips(recon, rows) + offset[None, :] - local
    resids = gather_chips(resid)
    (grad_part,) = call(
        functools.partial(gradient_kernel, len(resids)),
        [((tokens, 2 * width), F32)],
        (*resids, high, low, norms),
        work,
        "gradient",
    )
    code_grad = sum(from_layers(grad_part)[1:], grad_part)
    pre_grad = code_grad * gate
    theirs = to_partner(pre_grad[:, width:])
    grad, grad_bias = weight_gradient(turned, pre_grad[:, :width], theirs)
    return (grad[None, :, :], grad_bias[0])


def solution(mesh):
    layers, latents = mesh.shape["layer"], mesh.shape["latent"]

    def body(*args):
        return on_device(layers, latents, *args)

    return jax.shard_map(
        body,
        mesh=mesh,
        in_specs=(
            P("layer", "latent", None),
            P("layer", None, "latent"),
            P("latent"),
            P("latent", "layer", None),
            P("layer", None),
        ),
        out_specs=(P("layer", None, "latent"), P("latent")),
        check_vma=False,
    )
```

```python
import functools

import jax
import jax.numpy as jnp
from jax import lax
from jax.experimental import pallas as pl
from jax.experimental.pallas import tpu as pltpu
from jax.sharding import PartitionSpec as P


SHARP = 4.0
DIRECT_MAX = 8
CHUNK = 256
LANES, PAIR = 128, 16
LIMIT = 30 * 2**20
F32, BF16 = jnp.float32, jnp.bfloat16


def split(x):
    high = x.astype(BF16)
    return high, (x - high.astype(F32)).astype(BF16)


def stacked(x):
    return jnp.concatenate(split(x), axis=0)


def dot(a, b, dims):
    return lax.dot_general(a, b, (dims, ((), ())), preferred_element_type=F32)


def fold(x):
    half = x.shape[0] // 2
    return x[:half] + x[half:]


def call(kernel, outs, args, flops, scratch=()):
    outs = tuple(jax.ShapeDtypeStruct(*o) for o in outs)
    moved = sum(a.size * a.dtype.itemsize for a in args + outs)
    return call_in_vmem(kernel, outs, args, flops, moved, scratch)


def call_in_vmem(kernel, outs, args, flops, moved, scratch):
    return pl.pallas_call(
        kernel,
        out_shape=outs,
        in_specs=[pl.BlockSpec(memory_space=pltpu.VMEM)] * len(args),
        out_specs=[pl.BlockSpec(memory_space=pltpu.VMEM)] * len(outs),
        scratch_shapes=scratch,
        compiler_params=pltpu.CompilerParams(vmem_limit_bytes=LIMIT),
        cost_estimate=pl.CostEstimate(flops=flops, bytes_accessed=moved, transcendentals=0),
    )(*args)


def rows_of(refs):
    return jnp.concatenate([r[...] for r in refs], axis=0) if len(refs) > 1 else refs[0][...]


def encode_kernel(n, *refs):
    blocks, (own_high, own_low, other, out) = refs[:n], refs[n:]
    left = stacked(rows_of(blocks))
    width = other.shape[1]
    totals = [None, None]
    for start in range(0, other.shape[0], CHUNK):
        here = slice(start, start + CHUNK)
        part = left[:, here]
        rights = ((own_high[here, :], own_low[here, :]), split(other[here, :]))
        for at in range(2):
            for right in rights[at]:
                term = dot(part, right, ((1,), (0,)))
                totals[at] = term if totals[at] is None else totals[at] + term
    for at in range(2):
        out[:, at * width : (at + 1) * width] = fold(totals[at])


def prepare_kernel(own, other, high, low, high_turned, low_turned, norms, squares):
    features = high.shape[1]
    runs = features // LANES
    rows = own.shape[0] // runs
    for at, w in enumerate((own, other)):

        def group(g, carry, at=at, w=w):
            total = jnp.zeros((PAIR, LANES), F32)
            here = pl.ds(pl.multiple_of(at * rows + g * PAIR, PAIR), PAIR)
            for j in range(runs):
                x = w[pl.ds(g * (PAIR * runs) + j, PAIR, stride=runs), :]
                lanes = slice(j * LANES, (j + 1) * LANES)
                high[here, lanes], low[here, lanes] = split(x)
                total = total + x * x
            squares[here, :] = total
            return carry

        lax.fori_loop(0, rows // PAIR, group, 0)
    sums = lax.dot_general(
        jnp.ones((8, LANES), F32),
        squares[...],
        (((1,), (1,)), ((), ())),
        precision=lax.Precision.HIGHEST,
        preferred_element_type=F32,
    )
    norms[...] = jnp.sqrt(sums[:1])
    for start in range(0, features, CHUNK):
        here = slice(start, start + CHUNK)
        high_turned[here, :] = high[:, here].T
        low_turned[here, :] = low[:, here].T


def columns_of(refs):
    spans, first = [], 0
    for ref in refs:
        spans.append((ref, first, first + ref.shape[1]))
        first += ref.shape[1]
    return spans


def crossed(x, mask, rows):
    blocks = range(x.shape[0] // rows)
    return jnp.concatenate([x[(b ^ mask) * rows : ((b ^ mask) + 1) * rows] for b in blocks], axis=0)


def decode_kernel(n, *refs):
    parts, (bias, high, low, gate), outs = refs[:n], refs[n : n + 4], refs[n + 4 :]
    pre = parts[0][...]
    for p in parts[1:]:
        pre = pre + p[...]
    scaled = SHARP * (pre + bias[...])
    decay = jnp.exp(-jnp.abs(scaled))
    codes = (jnp.maximum(scaled, 0.0) + jnp.log1p(decay)) / SHARP
    gate[...] = jnp.where(scaled >= 0, 1.0, decay) / (1.0 + decay)
    left = stacked(codes)
    for start in range(0, high.shape[1], CHUNK):
        here = slice(start, start + CHUNK)
        share = fold(
            dot(left, high[:, here], ((1,), (0,))) + dot(left, low[:, here], ((1,), (0,)))
        )
        for out, first, last in columns_of(outs):
            low_end, high_end = max(start, first), min(start + CHUNK, last)
            if low_end < high_end:
                out[:, low_end - first : high_end - first] = share[
                    :, low_end - start : high_end - start
                ]


def gradient_kernel(n, masks, rows, *refs):
    blocks, (shift, high, low, norms), pieces, out = refs[:n], refs[n : n + 4], refs[n + 4 : -1], refs[-1]
    recon = []
    for mask in masks:
        held, *pieces = pieces
        total = held[...]
        if mask:
            other, *pieces = pieces
            total = total + crossed(other[...], mask, rows)
        recon.append(total)
    left = stacked(jnp.concatenate(recon, axis=1) + shift[...] - rows_of(blocks))
    total = None
    for start in range(0, high.shape[0], CHUNK):
        here = slice(start, start + CHUNK)
        for right in (high, low):
            term = dot(left[:, here], right[here, :], ((1,), (0,)))
            total = term if total is None else total + term
    out[...] = fold(total) + norms[...]


def turn_kernel(n, *refs):
    own, (other, out) = refs[:n], refs[n:]
    x = jnp.concatenate([rows_of(own), other[...]], axis=0)
    high, low = split(x)
    out[...] = jnp.concatenate([high, low, high, low], axis=0).T


def weight_kernel(tile, turned, mine, theirs, out, bias, right, result, sem):
    grad = jnp.concatenate([mine[...], theirs[...]], axis=0)
    bias[...] = jnp.sum(grad, axis=0, keepdims=True)
    high, low = split(grad)
    right[...] = jnp.concatenate([high, high, low, low], axis=0)
    copies = []
    for at in range(sem.shape[0]):
        here = slice(at * tile, (at + 1) * tile)
        result[here, :] = dot(turned[here, :], right[...], ((1,), (0,)))
        copies.append(pltpu.make_async_copy(result.at[here, :], out.at[here, :], sem.at[at]))
        copies[-1].start()
    for copy in copies:
        copy.wait()


def weight_gradient(turned, mine, theirs):
    features, depth = turned.shape
    width = mine.shape[1]
    steps = next(n for n in (6, 4, 3, 2, 1) if features % (8 * n) == 0)
    vmem = pl.BlockSpec(memory_space=pltpu.VMEM)
    return pl.pallas_call(
        functools.partial(weight_kernel, features // steps),
        out_shape=(
            jax.ShapeDtypeStruct((features, width), F32),
            jax.ShapeDtypeStruct((1, width), F32),
        ),
        in_specs=[vmem] * 3,
        out_specs=[pl.BlockSpec(memory_space=pltpu.HBM), vmem],
        scratch_shapes=[
            pltpu.VMEM((depth, width), BF16),
            pltpu.VMEM((features, width), F32),
            pltpu.SemaphoreType.DMA((steps,)),
        ],
        compiler_params=pltpu.CompilerParams(vmem_limit_bytes=LIMIT),
        cost_estimate=pl.CostEstimate(
            flops=2 * features * depth * width,
            bytes_accessed=features * (depth * 2 + width * 4),
            transcendentals=0,
        ),
        name="weight_gradient",
    )(turned, mine, theirs)


def on_device(layers, latents, acts, w_enc, b_enc, w_dec, b_dec):
    chips = latents // 2
    direct = chips <= DIRECT_MAX and chips & (chips - 1) == 0
    steps = chips.bit_length() - 1
    same_core = [[2 * j + c for j in range(chips)] for c in range(2)]

    def to_partner(x):
        return lax.ppermute(x, "latent", [(i, i ^ 1) for i in range(latents)])

    def to_chip(x, k):
        return lax.ppermute(x, "latent", [(i, i ^ (2 * k)) for i in range(latents)])

    def gather_chips(x):
        if direct:
            return [x] + [to_chip(x, k) for k in range(1, chips)]
        return [lax.all_gather(x, "latent", axis=0, tiled=True, axis_index_groups=same_core)]

    def sum_chips(shares, rows):
        if not direct or chips == 1:
            if not direct:
                shares = [lax.psum(x, "latent", axis_index_groups=same_core) for x in shares]
            return [0] * len(shares), list(shares)
        held, other = list(shares), [None] * len(shares)
        for step in range(steps):
            for at in range(len(held)):
                mask = 1 << ((step + at) % steps)
                if step:
                    before = 1 << ((step - 1 + at) % steps)
                    held[at] = held[at] + crossed(other[at], before, rows)
                other[at] = to_chip(held[at], mask)
        masks = [1 << ((steps - 1 + at) % steps) for at in range(len(held))]
        return masks, [x for pair in zip(held, other) for x in pair]

    def from_layers(x):
        near = list(range(1, layers))
        if layers == 4:
            orders = ((1, 3, 2), (3, 2, 1))
        else:
            orders = (near, near)
        got = [x]
        for step in range(layers - 1):
            pairs = []
            for layer in range(layers):
                for at in range(latents):
                    k = orders[at & 1][step]
                    to = layer ^ k if layers & (layers - 1) == 0 else (layer + k) % layers
                    pairs.append((layer * latents + at, to * latents + at))
            got.append(lax.ppermute(x, ("layer", "latent"), pairs))
        return got

    enc, local = w_enc[0], acts[0]
    rows, features = local.shape
    width = enc.shape[1]
    tokens = rows * chips
    work = 4 * 2 * tokens * features * 2 * width
    dec = w_dec.reshape(width * features // LANES, LANES)

    other_enc = to_partner(enc)
    other_dec = to_partner(dec)
    received = gather_chips(local)
    rounded = lax.reduce_precision(enc, 8, 7)
    own_high, own_low = rounded.astype(BF16), (enc - rounded).astype(BF16)
    gathered = received
    (partial,) = call(
        functools.partial(encode_kernel, len(gathered)),
        [((tokens, 2 * width), F32)],
        (*gathered, own_high, own_low, other_enc),
        work,
    )
    first = lax.optimization_barrier((b_enc, partial))[0]
    extra = jnp.pad(first[None, :], ((0, 7), (0, features - width)))
    packed = jnp.concatenate(gathered + [extra], axis=0)
    packed = to_partner(packed)
    high, low, high_turned, low_turned, norms = call(
        prepare_kernel,
        [((2 * width, features), BF16)] * 2
        + [((features, 2 * width), BF16)] * 2
        + [((1, 2 * width), F32)],
        (dec, other_dec),
        work,
        (pltpu.VMEM((2 * width, LANES), F32),),
    )
    parts, packed = lax.optimization_barrier((from_layers(partial), packed))
    bias = jnp.concatenate([b_enc, packed[tokens, :width]])[None, :]
    sets = steps if direct and steps > 1 and features % (steps * LANES) == 0 else 1
    gate, *shares = call(
        functools.partial(decode_kernel, len(parts)),
        [((tokens, 2 * width), F32)] + [((tokens, features // sets), F32)] * sets,
        (*parts, bias, high, low),
        work,
    )
    (turned,) = call(
        functools.partial(turn_kernel, len(gathered)),
        [((features, 8 * tokens), BF16)],
        (*gathered, packed[:tokens]),
        work,
    )
    masks, pieces = sum_chips(shares, rows)
    pieces, turned = lax.optimization_barrier((pieces, turned))
    (grad_part,) = call(
        functools.partial(gradient_kernel, len(gathered), masks, rows),
        [((tokens, 2 * width), F32)],
        (*gathered, b_dec, high_turned, low_turned, norms, *pieces),
        work,
    )
    code_grad = sum(from_layers(grad_part)[1:], grad_part)
    pre_grad = code_grad * gate
    theirs = to_partner(pre_grad[:, width:])
    grad, grad_bias = weight_gradient(turned, pre_grad[:, :width], theirs)
    return (grad[None, :, :], grad_bias[0])


def solution(mesh):
    layers, latents = mesh.shape["layer"], mesh.shape["latent"]

    def body(*args):
        return on_device(layers, latents, *args)

    return jax.shard_map(
        body,
        mesh=mesh,
        in_specs=(
            P("layer", "latent", None),
            P("layer", None, "latent"),
            P("latent"),
            P("latent", "layer", None),
            P("layer", None),
        ),
        out_specs=(P("layer", None, "latent"), P("latent")),
        check_vma=False,
    )
```

```python
import functools

import jax
import jax.numpy as jnp
from jax import lax
from jax.experimental import pallas as pl
from jax.experimental.pallas import tpu as pltpu
from jax.sharding import PartitionSpec as P


SHARP = 4.0
DIRECT_MAX = 8
CHUNK = 256
LANES, PAIR = 128, 16
LIMIT = 30 * 2**20
F32, BF16 = jnp.float32, jnp.bfloat16


def split(x):
    high = x.astype(BF16)
    return high, (x - high.astype(F32)).astype(BF16)


def stacked(x):
    return jnp.concatenate(split(x), axis=0)


def dot(a, b, dims):
    return lax.dot_general(a, b, (dims, ((), ())), preferred_element_type=F32)


def fold(x):
    half = x.shape[0] // 2
    return x[:half] + x[half:]


def call(kernel, outs, args, flops, scratch=()):
    outs = tuple(jax.ShapeDtypeStruct(*o) for o in outs)
    moved = sum(a.size * a.dtype.itemsize for a in args + outs)
    return call_in_vmem(kernel, outs, args, flops, moved, scratch)


def call_in_vmem(kernel, outs, args, flops, moved, scratch):
    return pl.pallas_call(
        kernel,
        out_shape=outs,
        in_specs=[pl.BlockSpec(memory_space=pltpu.VMEM)] * len(args),
        out_specs=[pl.BlockSpec(memory_space=pltpu.VMEM)] * len(outs),
        scratch_shapes=scratch,
        compiler_params=pltpu.CompilerParams(vmem_limit_bytes=LIMIT),
        cost_estimate=pl.CostEstimate(flops=flops, bytes_accessed=moved, transcendentals=0),
    )(*args)


def rows_of(refs):
    return jnp.concatenate([r[...] for r in refs], axis=0) if len(refs) > 1 else refs[0][...]


def encode_kernel(n, *refs):
    blocks, (own_high, own_low, other, out) = refs[:n], refs[n:]
    left = stacked(rows_of(blocks))
    width = other.shape[1]
    totals = [None, None]
    for start in range(0, other.shape[0], CHUNK):
        here = slice(start, start + CHUNK)
        part = left[:, here]
        rights = ((own_high[here, :], own_low[here, :]), split(other[here, :]))
        for at in range(2):
            for right in rights[at]:
                term = dot(part, right, ((1,), (0,)))
                totals[at] = term if totals[at] is None else totals[at] + term
    for at in range(2):
        out[:, at * width : (at + 1) * width] = fold(totals[at])


def prepare_kernel(own, other, high, low, high_turned, low_turned, norms, squares):
    features = high.shape[1]
    runs = features // LANES
    rows = own.shape[0] // runs
    for at, w in enumerate((own, other)):

        def group(g, carry, at=at, w=w):
            total = jnp.zeros((PAIR, LANES), F32)
            here = pl.ds(pl.multiple_of(at * rows + g * PAIR, PAIR), PAIR)
            for j in range(runs):
                x = w[pl.ds(g * (PAIR * runs) + j, PAIR, stride=runs), :]
                lanes = slice(j * LANES, (j + 1) * LANES)
                high[here, lanes], low[here, lanes] = split(x)
                total = total + x * x
            squares[here, :] = total
            return carry

        lax.fori_loop(0, rows // PAIR, group, 0)
    sums = lax.dot_general(
        jnp.ones((8, LANES), F32),
        squares[...],
        (((1,), (1,)), ((), ())),
        precision=lax.Precision.HIGHEST,
        preferred_element_type=F32,
    )
    norms[...] = jnp.sqrt(sums[:1])
    for start in range(0, features, CHUNK):
        here = slice(start, start + CHUNK)
        high_turned[here, :] = high[:, here].T
        low_turned[here, :] = low[:, here].T


def columns_of(refs):
    spans, first = [], 0
    for ref in refs:
        spans.append((ref, first, first + ref.shape[1]))
        first += ref.shape[1]
    return spans


def crossed(x, mask, rows):
    blocks = range(x.shape[0] // rows)
    return jnp.concatenate([x[(b ^ mask) * rows : ((b ^ mask) + 1) * rows] for b in blocks], axis=0)


def decode_kernel(n, *refs):
    parts, (bias, high, low, gate), outs = refs[:n], refs[n : n + 4], refs[n + 4 :]
    pre = parts[0][...]
    for p in parts[1:]:
        pre = pre + p[...]
    scaled = SHARP * (pre + bias[...])
    decay = jnp.exp(-jnp.abs(scaled))
    codes = (jnp.maximum(scaled, 0.0) + jnp.log1p(decay)) / SHARP
    gate[...] = jnp.where(scaled >= 0, 1.0, decay) / (1.0 + decay)
    left = stacked(codes)
    for start in range(0, high.shape[1], CHUNK):
        here = slice(start, start + CHUNK)
        share = fold(
            dot(left, high[:, here], ((1,), (0,))) + dot(left, low[:, here], ((1,), (0,)))
        )
        for out, first, last in columns_of(outs):
            low_end, high_end = max(start, first), min(start + CHUNK, last)
            if low_end < high_end:
                out[:, low_end - first : high_end - first] = share[
                    :, low_end - start : high_end - start
                ]


def gradient_kernel(n, masks, rows, *refs):
    blocks, (shift, high, low, norms), pieces, out = refs[:n], refs[n : n + 4], refs[n + 4 : -1], refs[-1]
    recon = []
    for mask in masks:
        held, *pieces = pieces
        total = held[...]
        if mask:
            other, *pieces = pieces
            total = total + crossed(other[...], mask, rows)
        recon.append(total)
    left = stacked(jnp.concatenate(recon, axis=1) + shift[...] - rows_of(blocks))
    total = None
    for start in range(0, high.shape[0], CHUNK):
        here = slice(start, start + CHUNK)
        for right in (high, low):
            term = dot(left[:, here], right[here, :], ((1,), (0,)))
            total = term if total is None else total + term
    out[...] = fold(total) + norms[...]


def turn_kernel(n, *refs):
    own, (other, out) = refs[:n], refs[n:]
    x = jnp.concatenate([rows_of(own), other[...]], axis=0)
    high, low = split(x)
    out[...] = jnp.concatenate([high, low, high, low], axis=0).T


def weight_kernel(tile, turned, mine, theirs, out, bias, right, result, sem):
    grad = jnp.concatenate([mine[...], theirs[...]], axis=0)
    bias[...] = jnp.sum(grad, axis=0, keepdims=True)
    high, low = split(grad)
    right[...] = jnp.concatenate([high, high, low, low], axis=0)
    copies = []
    for at in range(sem.shape[0]):
        here = slice(at * tile, (at + 1) * tile)
        result[here, :] = dot(turned[here, :], right[...], ((1,), (0,)))
        copies.append(pltpu.make_async_copy(result.at[here, :], out.at[here, :], sem.at[at]))
        copies[-1].start()
    for copy in copies:
        copy.wait()


def weight_gradient(turned, mine, theirs):
    features, depth = turned.shape
    width = mine.shape[1]
    steps = next(n for n in (6, 4, 3, 2, 1) if features % (8 * n) == 0)
    vmem = pl.BlockSpec(memory_space=pltpu.VMEM)
    return pl.pallas_call(
        functools.partial(weight_kernel, features // steps),
        out_shape=(
            jax.ShapeDtypeStruct((features, width), F32),
            jax.ShapeDtypeStruct((1, width), F32),
        ),
        in_specs=[vmem] * 3,
        out_specs=[pl.BlockSpec(memory_space=pltpu.HBM), vmem],
        scratch_shapes=[
            pltpu.VMEM((depth, width), BF16),
            pltpu.VMEM((features, width), F32),
            pltpu.SemaphoreType.DMA((steps,)),
        ],
        compiler_params=pltpu.CompilerParams(vmem_limit_bytes=LIMIT),
        cost_estimate=pl.CostEstimate(
            flops=2 * features * depth * width,
            bytes_accessed=features * (depth * 2 + width * 4),
            transcendentals=0,
        ),
        name="weight_gradient",
    )(turned, mine, theirs)


def on_device(layers, latents, acts, w_enc, b_enc, w_dec, b_dec):
    chips = latents // 2
    direct = chips <= DIRECT_MAX and chips & (chips - 1) == 0
    steps = chips.bit_length() - 1
    same_core = [[2 * j + c for j in range(chips)] for c in range(2)]

    def to_partner(x):
        return lax.ppermute(x, "latent", [(i, i ^ 1) for i in range(latents)])

    def to_chip(x, k):
        return lax.ppermute(x, "latent", [(i, i ^ (2 * k)) for i in range(latents)])

    def gather_chips(x):
        if direct:
            return [x] + [to_chip(x, k) for k in range(1, chips)]
        return [lax.all_gather(x, "latent", axis=0, tiled=True, axis_index_groups=same_core)]

    def sum_chips(shares, rows):
        if not direct or chips == 1:
            if not direct:
                shares = [lax.psum(x, "latent", axis_index_groups=same_core) for x in shares]
            return [0] * len(shares), list(shares)
        held, other = list(shares), [None] * len(shares)
        for step in range(steps):
            for at in range(len(held)):
                mask = 1 << ((step + at) % steps)
                if step:
                    before = 1 << ((step - 1 + at) % steps)
                    held[at] = held[at] + crossed(other[at], before, rows)
                other[at] = to_chip(held[at], mask)
        masks = [1 << ((steps - 1 + at) % steps) for at in range(len(held))]
        return masks, [x for pair in zip(held, other) for x in pair]

    def from_layers(x):
        got = [x]
        for step in range(layers - 1):
            k = layers - 1 if step == 0 else step
            even = layers & (layers - 1) == 0
            pairs = [(i, i ^ k if even else (i + k) % layers) for i in range(layers)]
            got.append(lax.ppermute(x, "layer", pairs))
        return got

    enc, local = w_enc[0], acts[0]
    rows, features = local.shape
    width = enc.shape[1]
    tokens = rows * chips
    work = 4 * 2 * tokens * features * 2 * width
    dec = w_dec.reshape(width * features // LANES, LANES)

    other_enc = to_partner(enc)
    other_dec = to_partner(dec)
    received = gather_chips(local)
    rounded = lax.reduce_precision(enc, 8, 7)
    own_high, own_low = rounded.astype(BF16), (enc - rounded).astype(BF16)
    gathered = received
    (partial,) = call(
        functools.partial(encode_kernel, len(gathered)),
        [((tokens, 2 * width), F32)],
        (*gathered, own_high, own_low, other_enc),
        work,
    )
    first = lax.optimization_barrier((b_enc, partial))[0]
    extra = jnp.pad(first[None, :], ((0, 7), (0, features - width)))
    packed = jnp.concatenate(gathered + [extra], axis=0)
    packed = to_partner(packed)
    high, low, high_turned, low_turned, norms = call(
        prepare_kernel,
        [((2 * width, features), BF16)] * 2
        + [((features, 2 * width), BF16)] * 2
        + [((1, 2 * width), F32)],
        (dec, other_dec),
        work,
        (pltpu.VMEM((2 * width, LANES), F32),),
    )
    parts, packed = lax.optimization_barrier((from_layers(partial), packed))
    bias = jnp.concatenate([b_enc, packed[tokens, :width]])[None, :]
    sets = steps if direct and steps > 1 and features % (steps * LANES) == 0 else 1
    gate, *shares = call(
        functools.partial(decode_kernel, len(parts)),
        [((tokens, 2 * width), F32)] + [((tokens, features // sets), F32)] * sets,
        (*parts, bias, high, low),
        work,
    )
    (turned,) = call(
        functools.partial(turn_kernel, len(gathered)),
        [((features, 8 * tokens), BF16)],
        (*gathered, packed[:tokens]),
        work,
    )
    masks, pieces = sum_chips(shares, rows)
    pieces, turned = lax.optimization_barrier((pieces, turned))
    (grad_part,) = call(
        functools.partial(gradient_kernel, len(gathered), masks, rows),
        [((tokens, 2 * width), F32)],
        (*gathered, b_dec, high_turned, low_turned, norms, *pieces),
        work,
    )
    code_grad = sum(from_layers(grad_part)[1:], grad_part)
    pre_grad = code_grad * gate
    theirs = to_partner(pre_grad[:, width:])
    grad, grad_bias = weight_gradient(turned, pre_grad[:, :width], theirs)
    return (grad[None, :, :], grad_bias[0])


def solution(mesh):
    layers, latents = mesh.shape["layer"], mesh.shape["latent"]

    def body(*args):
        return on_device(layers, latents, *args)

    return jax.shard_map(
        body,
        mesh=mesh,
        in_specs=(
            P("layer", "latent", None),
            P("layer", None, "latent"),
            P("latent"),
            P("latent", "layer", None),
            P("layer", None),
        ),
        out_specs=(P("layer", None, "latent"), P("latent")),
        check_vma=False,
    )
```

```python
import functools

import jax
import jax.numpy as jnp
from jax import lax
from jax.experimental import pallas as pl
from jax.experimental.pallas import tpu as pltpu
from jax.sharding import PartitionSpec as P


SHARP = 4.0
DIRECT_MAX = 8
CHUNK = 256
LANES, PAIR = 128, 16
LIMIT = 30 * 2**20
F32, BF16 = jnp.float32, jnp.bfloat16


def split(x):
    high = x.astype(BF16)
    return high, (x - high.astype(F32)).astype(BF16)


def stacked(x):
    return jnp.concatenate(split(x), axis=0)


def dot(a, b, dims):
    return lax.dot_general(a, b, (dims, ((), ())), preferred_element_type=F32)


def fold(x):
    half = x.shape[0] // 2
    return x[:half] + x[half:]


def call(kernel, outs, args, flops, scratch=()):
    outs = tuple(jax.ShapeDtypeStruct(*o) for o in outs)
    moved = sum(a.size * a.dtype.itemsize for a in args + outs)
    return call_in_vmem(kernel, outs, args, flops, moved, scratch)


def call_in_vmem(kernel, outs, args, flops, moved, scratch):
    return pl.pallas_call(
        kernel,
        out_shape=outs,
        in_specs=[pl.BlockSpec(memory_space=pltpu.VMEM)] * len(args),
        out_specs=[pl.BlockSpec(memory_space=pltpu.VMEM)] * len(outs),
        scratch_shapes=scratch,
        compiler_params=pltpu.CompilerParams(vmem_limit_bytes=LIMIT),
        cost_estimate=pl.CostEstimate(flops=flops, bytes_accessed=moved, transcendentals=0),
    )(*args)


def rows_of(refs):
    return jnp.concatenate([r[...] for r in refs], axis=0) if len(refs) > 1 else refs[0][...]


def encode_kernel(n, *refs):
    blocks, (own_high, own_low, other, out) = refs[:n], refs[n:]
    left = stacked(rows_of(blocks))
    width = other.shape[1]
    totals = [None, None]
    for start in range(0, other.shape[0], 768):
        here = slice(start, start + 768)
        part = left[:, here]
        rights = ((own_high[here, :], own_low[here, :]), split(other[here, :]))
        for at in range(2):
            for right in rights[at]:
                term = dot(part, right, ((1,), (0,)))
                totals[at] = term if totals[at] is None else totals[at] + term
    for at in range(2):
        out[:, at * width : (at + 1) * width] = fold(totals[at])


def prepare_kernel(own, other, high, low, high_turned, low_turned, norms, squares):
    features = high.shape[1]
    runs = features // LANES
    rows = own.shape[0] // runs
    for at, w in enumerate((own, other)):

        def group(g, carry, at=at, w=w):
            total = jnp.zeros((PAIR, LANES), F32)
            here = pl.ds(pl.multiple_of(at * rows + g * PAIR, PAIR), PAIR)
            for j in range(runs):
                x = w[pl.ds(g * (PAIR * runs) + j, PAIR, stride=runs), :]
                lanes = slice(j * LANES, (j + 1) * LANES)
                high[here, lanes], low[here, lanes] = split(x)
                total = total + x * x
            squares[here, :] = total
            return carry

        lax.fori_loop(0, rows // PAIR, group, 0)
    sums = lax.dot_general(
        jnp.ones((8, LANES), F32),
        squares[...],
        (((1,), (1,)), ((), ())),
        precision=lax.Precision.HIGHEST,
        preferred_element_type=F32,
    )
    norms[...] = jnp.sqrt(sums[:1])
    for start in range(0, features, CHUNK):
        here = slice(start, start + CHUNK)
        high_turned[here, :] = high[:, here].T
        low_turned[here, :] = low[:, here].T


def columns_of(refs):
    spans, first = [], 0
    for ref in refs:
        spans.append((ref, first, first + ref.shape[1]))
        first += ref.shape[1]
    return spans


def crossed(x, mask, rows):
    blocks = range(x.shape[0] // rows)
    return jnp.concatenate([x[(b ^ mask) * rows : ((b ^ mask) + 1) * rows] for b in blocks], axis=0)


def decode_kernel(n, *refs):
    parts, (bias, high, low, gate), outs = refs[:n], refs[n : n + 4], refs[n + 4 :]
    pre = parts[0][...]
    for p in parts[1:]:
        pre = pre + p[...]
    scaled = SHARP * (pre + bias[...])
    decay = jnp.exp(-jnp.abs(scaled))
    codes = (jnp.maximum(scaled, 0.0) + jnp.log1p(decay)) / SHARP
    gate[...] = jnp.where(scaled >= 0, 1.0, decay) / (1.0 + decay)
    left = stacked(codes)
    for start in range(0, high.shape[1], CHUNK):
        here = slice(start, start + CHUNK)
        share = fold(
            dot(left, high[:, here], ((1,), (0,))) + dot(left, low[:, here], ((1,), (0,)))
        )
        for out, first, last in columns_of(outs):
            low_end, high_end = max(start, first), min(start + CHUNK, last)
            if low_end < high_end:
                out[:, low_end - first : high_end - first] = share[
                    :, low_end - start : high_end - start
                ]


def gradient_kernel(n, masks, rows, *refs):
    blocks, (shift, high, low, norms), pieces, out = refs[:n], refs[n : n + 4], refs[n + 4 : -1], refs[-1]
    recon = []
    for mask in masks:
        held, *pieces = pieces
        total = held[...]
        if mask:
            other, *pieces = pieces
            total = total + crossed(other[...], mask, rows)
        recon.append(total)
    left = stacked(jnp.concatenate(recon, axis=1) + shift[...] - rows_of(blocks))
    total = None
    for start in range(0, high.shape[0], CHUNK):
        here = slice(start, start + CHUNK)
        for right in (high, low):
            term = dot(left[:, here], right[here, :], ((1,), (0,)))
            total = term if total is None else total + term
    out[...] = fold(total) + norms[...]


def turn_kernel(n, *refs):
    own, (other, out) = refs[:n], refs[n:]
    x = jnp.concatenate([rows_of(own), other[...]], axis=0)
    high, low = split(x)
    out[...] = jnp.concatenate([high, low, high, low], axis=0).T


def weight_kernel(tile, turned, mine, theirs, out, bias, right, result, sem):
    grad = jnp.concatenate([mine[...], theirs[...]], axis=0)
    bias[...] = jnp.sum(grad, axis=0, keepdims=True)
    high, low = split(grad)
    right[...] = jnp.concatenate([high, high, low, low], axis=0)
    copies = []
    for at in range(sem.shape[0]):
        here = slice(at * tile, (at + 1) * tile)
        result[here, :] = dot(turned[here, :], right[...], ((1,), (0,)))
        copies.append(pltpu.make_async_copy(result.at[here, :], out.at[here, :], sem.at[at]))
        copies[-1].start()
    for copy in copies:
        copy.wait()


def weight_gradient(turned, mine, theirs):
    features, depth = turned.shape
    width = mine.shape[1]
    steps = next(n for n in (3, 2, 1) if features % (8 * n) == 0)
    vmem = pl.BlockSpec(memory_space=pltpu.VMEM)
    return pl.pallas_call(
        functools.partial(weight_kernel, features // steps),
        out_shape=(
            jax.ShapeDtypeStruct((features, width), F32),
            jax.ShapeDtypeStruct((1, width), F32),
        ),
        in_specs=[vmem] * 3,
        out_specs=[pl.BlockSpec(memory_space=pltpu.HBM), vmem],
        scratch_shapes=[
            pltpu.VMEM((depth, width), BF16),
            pltpu.VMEM((features, width), F32),
            pltpu.SemaphoreType.DMA((steps,)),
        ],
        compiler_params=pltpu.CompilerParams(vmem_limit_bytes=LIMIT),
        cost_estimate=pl.CostEstimate(
            flops=2 * features * depth * width,
            bytes_accessed=features * (depth * 2 + width * 4),
            transcendentals=0,
        ),
        name="weight_gradient",
    )(turned, mine, theirs)


def on_device(layers, latents, acts, w_enc, b_enc, w_dec, b_dec):
    chips = latents // 2
    direct = chips <= DIRECT_MAX and chips & (chips - 1) == 0
    steps = chips.bit_length() - 1
    same_core = [[2 * j + c for j in range(chips)] for c in range(2)]

    def to_partner(x):
        return lax.ppermute(x, "latent", [(i, i ^ 1) for i in range(latents)])

    def to_chip(x, k):
        return lax.ppermute(x, "latent", [(i, i ^ (2 * k)) for i in range(latents)])

    def gather_chips(x):
        if direct:
            return [x] + [to_chip(x, k) for k in range(1, chips)]
        return [lax.all_gather(x, "latent", axis=0, tiled=True, axis_index_groups=same_core)]

    def sum_chips(shares, rows):
        if not direct or chips == 1:
            if not direct:
                shares = [lax.psum(x, "latent", axis_index_groups=same_core) for x in shares]
            return [0] * len(shares), list(shares)
        held, other = list(shares), [None] * len(shares)
        for step in range(steps):
            for at in range(len(held)):
                mask = 1 << ((step + at) % steps)
                if step:
                    before = 1 << ((step - 1 + at) % steps)
                    held[at] = held[at] + crossed(other[at], before, rows)
                other[at] = to_chip(held[at], mask)
        masks = [1 << ((steps - 1 + at) % steps) for at in range(len(held))]
        return masks, [x for pair in zip(held, other) for x in pair]

    def from_layers(x):
        got = [x]
        for step in range(layers - 1):
            k = layers - 1 if step == 0 else step
            even = layers & (layers - 1) == 0
            pairs = [(i, i ^ k if even else (i + k) % layers) for i in range(layers)]
            got.append(lax.ppermute(x, "layer", pairs))
        return got

    enc, local = w_enc[0], acts[0]
    rows, features = local.shape
    width = enc.shape[1]
    tokens = rows * chips
    work = 4 * 2 * tokens * features * 2 * width
    dec = w_dec.reshape(width * features // LANES, LANES)

    other_enc = to_partner(enc)
    other_dec = to_partner(dec)
    received = gather_chips(local)
    rounded = lax.reduce_precision(enc, 8, 7)
    own_high, own_low = rounded.astype(BF16), (enc - rounded).astype(BF16)
    gathered = received
    (partial,) = call(
        functools.partial(encode_kernel, len(gathered)),
        [((tokens, 2 * width), F32)],
        (*gathered, own_high, own_low, other_enc),
        work,
    )
    first = lax.optimization_barrier((b_enc, partial))[0]
    extra = jnp.pad(first[None, :], ((0, 7), (0, features - width)))
    packed = jnp.concatenate(gathered + [extra], axis=0)
    packed = to_partner(packed)
    high, low, high_turned, low_turned, norms = call(
        prepare_kernel,
        [((2 * width, features), BF16)] * 2
        + [((features, 2 * width), BF16)] * 2
        + [((1, 2 * width), F32)],
        (dec, other_dec),
        work,
        (pltpu.VMEM((2 * width, LANES), F32),),
    )
    parts, packed = lax.optimization_barrier((from_layers(partial), packed))
    bias = jnp.concatenate([b_enc, packed[tokens, :width]])[None, :]
    sets = steps if direct and steps > 1 and features % (steps * LANES) == 0 else 1
    gate, *shares = call(
        functools.partial(decode_kernel, len(parts)),
        [((tokens, 2 * width), F32)] + [((tokens, features // sets), F32)] * sets,
        (*parts, bias, high, low),
        work,
    )
    (turned,) = call(
        functools.partial(turn_kernel, len(gathered)),
        [((features, 8 * tokens), BF16)],
        (*gathered, packed[:tokens]),
        work,
    )
    masks, pieces = sum_chips(shares, rows)
    (grad_part,) = call(
        functools.partial(gradient_kernel, len(gathered), masks, rows),
        [((tokens, 2 * width), F32)],
        (*gathered, b_dec, high_turned, low_turned, norms, *pieces),
        work,
    )
    code_grad = sum(from_layers(grad_part)[1:], grad_part)
    pre_grad = code_grad * gate
    theirs = to_partner(pre_grad[:, width:])
    grad, grad_bias = weight_gradient(turned, pre_grad[:, :width], theirs)
    return (grad[None, :, :], grad_bias[0])


def solution(mesh):
    layers, latents = mesh.shape["layer"], mesh.shape["latent"]

    def body(*args):
        return on_device(layers, latents, *args)

    return jax.shard_map(
        body,
        mesh=mesh,
        in_specs=(
            P("layer", "latent", None),
            P("layer", None, "latent"),
            P("latent"),
            P("latent", "layer", None),
            P("layer", None),
        ),
        out_specs=(P("layer", None, "latent"), P("latent")),
        check_vma=False,
    )
```
